32 devices in a mesh: gx: 4 (over x, core), gy: 8 (over z, y).
Axes of the slice: x: 2, y: 2, z: 4, core: 2. Of those that a mesh axis runs over, the one named last changes fastest.
Arguments:
- state: float32 [512, 512, 128], P('gx', 'gy'), may hold values from -6 to 6
- diffusion: float32 [512, 512, 128], P('gx', 'gy'), may hold values from 0.01 to 0.12
- vert_inverse: float32 [512, 128, 128], P('gy'), as said below
- profiles: bfloat16 [8192, 128], P(('gx', 'gy')), may hold values from -6 to 6
- counts: int32 [32, 32], P(('gx', 'gy')), may hold values from 0 to 16, as said below
- cell_lon: int32 [8192], P(('gx', 'gy')), may hold values from 0 to 127
- cell_lat: int32 [8192], P(('gx', 'gy')), may hold values from 0 to 63
- weight_slot: int32 [2, 8192], P(None, ('gx', 'gy')), may hold values from 0 to 63
Outputs:
- adjoint: float32 [512, 512, 128], P('gx', 'gy')
The draws below stay inside these ranges and needn't reach their ends.
Inputs may be any that keep to these rules, and one draw needn't show every extreme that they name: Each row s sums to 256; source device s stores its profiles in order of subdomain, counts[s,d] of them for subdomain d, which covers longitude cells (d // 8) * 128 onwards and latitude cells (d % 8) * 64 onwards. Some subdomain receives 16 profiles from every source. `vert_inverse`: one matrix for each latitude row.
All inputs are finite; a program needn't handle non-finite values.
Results may differ from the reference program's by a relative error of at most 0.0015.
Values may be sent and summed in bfloat16 or wider, within the bound.
A program may use at most 128 MiB of HBM per device.

```python
import math
import jax
import jax.numpy as jnp
from jax import lax

L = 128
CX = 128
CY = 64
CAP = 16
STEPS = 4
SLOTS = 64
NX = 512
NY = 512
OBS = 8192
N_GX = 4
N_GY = 8
DEVICES = 32


def draw_vert_inverse(key, part):
    shape = (NY, L, L)
    noise = jax.random.normal(key, shape, jnp.float32)
    return 0.9 * jnp.eye(L, dtype=jnp.float32)[None] + 0.4 * noise / jnp.sqrt(jnp.float32(L))


def draw_counts(key, part):
    half = CAP // 2
    key_heavy = jax.random.fold_in(key, 11)
    key_rows = jax.random.fold_in(key, 12)
    heavy = jax.random.randint(key_heavy, (), 0, DEVICES)
    ids = jnp.arange(DEVICES, dtype=jnp.int32)

    def one_row(row_key):
        key_perm = jax.random.fold_in(row_key, 1)
        key_amount = jax.random.fold_in(row_key, 2)
        order = jax.random.permutation(key_perm, DEVICES).astype(jnp.int32)
        where_heavy = jnp.sum(jnp.where(order == heavy, ids, 0))
        first = order[0]
        order = order.at[where_heavy].set(first).at[0].set(heavy)
        amount = jax.random.randint(key_amount, (DEVICES // 2,), 0, half + 1).astype(jnp.int32)
        amount = amount.at[0].set(half)
        paired = jnp.stack([amount, -amount], axis=1).reshape(DEVICES)
        change = jnp.zeros((DEVICES,), jnp.int32).at[order].set(paired)
        return half + change
    row_keys = jax.random.split(key_rows, DEVICES)
    return jax.vmap(one_row)(row_keys).astype(jnp.int32)


def place_ends(result, stream_key, low, high):
    place = [jax.random.randint(jax.random.fold_in(stream_key, axis), (), 0, length) for axis, length in enumerate(result.shape)]
    widest = result.shape.index(max(result.shape))
    neighbour = place[:widest] + [(place[widest] + 1) % result.shape[widest]] + place[widest + 1:]
    return result.at[tuple(place)].set(low).at[tuple(neighbour)].set(high)


def block_scale(stream_key, extent, cuts, least, top_value):
    def one(axis_at, shards_of):
        draws = jax.random.uniform(jax.random.fold_in(jax.random.fold_in(stream_key, 6), axis_at), (shards_of,), jnp.float32, least / len(cuts), top_value / len(cuts))
        return jnp.repeat(jnp.exp(draws), extent[axis_at] // shards_of).reshape((-1,) + (1,) * (len(extent) - axis_at - 1))

    level = one(*cuts[0])
    for cut in cuts[1:]:
        level = level * one(*cut)
    return level


def gaussian(rng, dims, width, limit, pieces=(), kind=jnp.bfloat16):
    values = width * jax.random.normal(rng, dims, jnp.float32)
    if pieces:
        values = values * block_scale(rng, dims, pieces, -0.22, 0.18)
    return jnp.clip(values, -limit, limit).astype(kind)


def setup_inputs(seed: int = 0) -> dict:
    streams_of = jax.random.split(jax.random.key(seed), 9)
    state = gaussian(streams_of[0], (NX, NY, L), 1.0, 6.0, ((0, 4), (1, 8)), jnp.float32)
    diffusion = jnp.clip(jnp.exp(math.log(0.12) - 2.4849066 * jax.random.uniform(streams_of[1], (NX, NY, L), jnp.float32) ** block_scale(streams_of[1], (NX, NY, L), ((0, 4), (1, 8)), -0.2, 0.2)), 0.01, 0.12)
    vert_inverse = draw_vert_inverse(jax.random.fold_in(streams_of[8], 71), 0)
    profiles = gaussian(streams_of[3], (OBS, L), 1.0, 6.0, ((0, 32),))
    counts = draw_counts(jax.random.fold_in(streams_of[8], 71), 0)
    cell_lon = place_ends(jax.random.randint(streams_of[5], (OBS,), 0, CX), jax.random.fold_in(streams_of[5], 1), 0, CX - 1).astype(jnp.int32)
    cell_lat = place_ends(jax.random.randint(streams_of[6], (OBS,), 0, CY), jax.random.fold_in(streams_of[6], 1), 0, CY - 1).astype(jnp.int32)
    weight_slot = place_ends(jax.random.randint(streams_of[7], (2, OBS), 0, SLOTS), jax.random.fold_in(streams_of[7], 1), 0, SLOTS - 1).astype(jnp.int32)
    return {"state": state, "diffusion": diffusion, "vert_inverse": vert_inverse, "profiles": profiles, "counts": counts, "cell_lon": cell_lon, "cell_lat": cell_lat, "weight_slot": weight_slot}


def reference(state, diffusion, vert_inverse, profiles, counts, cell_lon, cell_lat, weight_slot):
    devices = N_GX * N_GY
    obs_dev = profiles.shape[0] // devices
    cumulative = jnp.cumsum(counts, axis=1)
    positions = jnp.arange(obs_dev, dtype=jnp.int32)
    owner = jax.vmap(lambda row: jnp.searchsorted(row, positions, side="right"))(cumulative)
    owner = owner.reshape(-1).astype(jnp.int32)
    lon_glob = (owner // N_GY) * CX + cell_lon
    lat_glob = (owner % N_GY) * CY + cell_lat
    frac_x = weight_slot[0].astype(jnp.float32) / SLOTS
    frac_y = weight_slot[1].astype(jnp.float32) / SLOTS
    lon_next = (lon_glob + 1) % NX
    lat_next = lat_glob + 1
    inside = (lat_next < NY).astype(jnp.float32)
    lat_next = jnp.minimum(lat_next, NY - 1)
    targets = jnp.concatenate([lon_glob * NY + lat_glob, lon_next * NY + lat_glob,
                               lon_glob * NY + lat_next, lon_next * NY + lat_next])
    weights = jnp.concatenate([(1.0 - frac_x) * (1.0 - frac_y), frac_x * (1.0 - frac_y),
                               (1.0 - frac_x) * frac_y * inside, frac_x * frac_y * inside])
    values = profiles.astype(jnp.float32)
    terms = weights[:, None] * jnp.concatenate([values, values, values, values])
    forcing = jax.ops.segment_sum(terms, targets, num_segments=NX * NY).reshape(NX, NY, -1)
    lam = state + forcing
    for section in range(STEPS):
        mixed = jnp.einsum("xym,ymk->xyk", lam, vert_inverse, precision=lax.Precision.HIGHEST)
        flux = diffusion * mixed
        padded = jnp.pad(flux, ((0, 0), (1, 1), (0, 0)))
        nearby = jnp.roll(flux, 1, axis=0) + jnp.roll(flux, -1, axis=0) + padded[:, 2:] + padded[:, :-2]
        lam = mixed + nearby - 4.0 * flux
    return lam
```

```python
import functools

import jax
import jax.numpy as jnp
from jax import lax
from jax.experimental import pallas as pl
from jax.experimental.pallas import tpu as pltpu
from jax.sharding import PartitionSpec as P

CAP = 16
STEPS = 4
SLOTS = 64
PAD = 8
ROWS = 8
FIELDS = 4
F32 = jnp.float32
BF16 = jnp.bfloat16
MESH = pl.DeviceIdType.MESH
VMEM_LIMIT = 60 * 1024 * 1024


def split(value):
    upper = value.astype(BF16)
    return upper, (value - upper.astype(F32)).astype(BF16)


def iota(shape, axis):
    return lax.broadcasted_iota(jnp.int32, shape, axis)


def kernel(
    n_gx, n_gy,
    prof_ref, counts_ref, lon_ref, lat_ref, slot_ref, state_hbm, diff_hbm, inv_hbm, out_hbm,
    st, df, wf, wst, fb, obuf, msg, mmsg, recv, mrecv, wx, upper, lower,
    col_send, col_recv, row_send, row_recv, corner_send, corner_recv,
    xs, xr, ys, yr,
    w_sem, st_sem, df_sem, out_sem, v_send, v_recv, m_send, m_recv,
    f_send, f_recv, x_send, x_recv, y_send, y_recv,
):
    lon, lat, levels = state_hbm.shape
    n_all = n_gx * n_gy
    slots = n_all * CAP
    obs = prof_ref.shape[0]
    blocks = lat // ROWS
    wide = lon + 2 * PAD
    gx, gy = lax.axis_index("gx"), lax.axis_index("gy")
    me = gx * n_gy + gy
    gx_up, gx_down = lax.rem(gx + 1, n_gx), lax.rem(gx + n_gx - 1, n_gx)
    gy_up, gy_down = lax.rem(gy + 1, n_gy), lax.rem(gy + n_gy - 1, n_gy)
    east, west, north, south = (gx_up, gy), (gx_down, gy), (gx, gy_up), (gx, gy_down)

    def peer(k):
        offset = jnp.where(k % 2 == 1, (k + 1) // 2, n_all - k // 2)
        other = lax.rem(me + offset, n_all)
        return other, (other // n_gy, lax.rem(other, n_gy))

    barrier = pltpu.get_barrier_semaphore()

    def greet(k, carry):
        pl.semaphore_signal(barrier, inc=1, device_id=peer(k)[1], device_id_type=MESH)
        return carry

    lax.fori_loop(1, n_all, greet, 0)

    def block_rows(b, pitch=lon):
        return pl.ds(b * ROWS * pitch, ROWS * pitch)

    w_loads = [
        pltpu.make_async_copy(
            inv_hbm.at[pl.ds(b * ROWS, ROWS)], wf.at[pl.ds(b * ROWS, ROWS)], w_sem.at[b]
        )
        for b in range(blocks)
    ]
    for load in w_loads:
        load.start()
    for y in range(lat):
        rows = pl.ds(y * lon, lon)
        pltpu.make_async_copy(state_hbm.at[:, y, :], st.at[rows], st_sem.at[y]).start()
    for y in range(lat):
        rows = pl.ds(y * lon, lon)
        pltpu.make_async_copy(diff_hbm.at[:, y, :], df.at[rows], df_sem.at[y]).start()

    count_row = counts_ref[...].astype(F32)
    dest, lane = iota((n_all, n_all), 0), iota((n_all, n_all), 1)
    start = jnp.sum(jnp.where(lane < dest, count_row, 0.0), axis=1, keepdims=True)
    count = jnp.sum(jnp.where(lane == dest, count_row, 0.0), axis=1, keepdims=True)
    position = iota((n_all, obs), 1).astype(F32)
    inside = jnp.where((position >= start) & (position < start + count), 1.0, 0.0)
    owner = iota((n_all, obs), 0).astype(F32)
    slot_of = jnp.sum(inside * (position - start), axis=0, keepdims=True)
    code = jnp.sum(inside * owner, axis=0, keepdims=True) * CAP + slot_of
    selector = jnp.where(iota((slots, obs), 0) == code.astype(jnp.int32), 1.0, 0.0).astype(BF16)
    msg[...] = (
        jnp.dot(selector, prof_ref[...], preferred_element_type=F32)
        .astype(BF16)
        .reshape(n_all, CAP, levels)
    )
    field = iota((levels, obs), 0)
    meta = jnp.where(field < CAP, lon_ref[...].astype(F32), lat_ref[...].astype(F32))
    meta = jnp.where(field < 2 * CAP, meta, slot_ref[0:1, :].astype(F32))
    meta = jnp.where(field < 3 * CAP, meta, slot_ref[1:2, :].astype(F32))
    meta = jnp.where(field % CAP == slot_of.astype(jnp.int32), meta, 0.0).astype(BF16)
    mmsg[...] = lax.dot_general(
        inside.astype(BF16), meta, (((1,), (1,)), ((), ())), preferred_element_type=F32
    ).reshape(n_all, 1, levels)

    pl.semaphore_wait(barrier, n_all - 1)

    def block_copies(k):
        other, device = peer(k)
        return (
            pltpu.make_async_remote_copy(
                src_ref=msg.at[other], dst_ref=recv.at[k],
                send_sem=v_send.at[k], recv_sem=v_recv.at[k],
                device_id=device, device_id_type=MESH,
            ),
            pltpu.make_async_remote_copy(
                src_ref=mmsg.at[other], dst_ref=mrecv.at[k],
                send_sem=m_send.at[k], recv_sem=m_recv.at[k],
                device_id=device, device_id_type=MESH,
            ),
        )

    def send(k, carry):
        for copy in block_copies(k):
            copy.start()
        return carry

    lax.fori_loop(1, n_all, send, 0)
    recv[0] = msg[me]
    mrecv[0] = mmsg[me]

    for b in range(blocks):
        w_loads[b].wait()

        def pairs(i, carry):
            for j in range(2):
                y = b * ROWS + 2 * i + j
                wst[y] = jnp.concatenate(split(wf[y]), axis=1)
            return carry

        lax.fori_loop(0, ROWS // 2, pairs, 0)

    for y in range(lat):
        rows = pl.ds(y * lon, lon)
        pltpu.make_async_copy(state_hbm.at[:, y, :], st.at[rows], st_sem.at[y]).wait()
    st[lat * lon :, :] = jnp.zeros((lon, levels), F32)

    def arrive(k, carry):
        for copy in block_copies(k):
            copy.wait_recv()
        return carry

    lax.fori_loop(1, n_all, arrive, 0)

    table = mrecv[...].reshape(n_all, levels)
    spread = jnp.where(iota((n_all, slots), 1) // CAP == iota((n_all, slots), 0), 1.0, 0.0)
    wide_table = lax.dot_general(
        table.astype(BF16), spread.astype(BF16), (((0,), (0,)), ((), ())),
        preferred_element_type=F32,
    )
    own = iota((levels, slots), 0) % CAP == iota((levels, slots), 1) % CAP
    wide_table = jnp.where(own, wide_table, 0.0)
    lon_row, lat_row, frac_row = [
        jnp.sum(wide_table[f * CAP : (f + 1) * CAP], axis=0, keepdims=True) for f in range(3)
    ]
    frac_row = frac_row / SLOTS
    x_ids = iota((lon, slots), 0).astype(F32)
    wx_f = jnp.where(x_ids == lon_row, 1.0 - frac_row, 0.0) + jnp.where(
        x_ids == lon_row + 1.0, frac_row, 0.0
    )
    wx[...] = wx_f.astype(BF16)
    pick = iota((CAP, levels), 1) - 3 * CAP == iota((CAP, levels), 0)

    for k in range(n_all):
        here = slice(k * CAP, (k + 1) * CAP)
        frac_y = (
            jnp.sum(jnp.where(pick, mrecv[k], 0.0), axis=1, keepdims=True) / SLOTS
        )
        values = recv[k].astype(F32)
        far = values * frac_y
        near_terms, far_terms = split(values - far), split(far)
        upper[here, 0:levels], lower[here, 0:levels] = near_terms
        upper[here, levels:], lower[here, levels:] = far_terms

    def weighted(rows):
        return jnp.dot(rows, upper[...], preferred_element_type=F32) + jnp.dot(
            rows, lower[...], preferred_element_type=F32
        )

    last = jnp.where(lon_row == lon - 1.0, frac_row, 0.0)
    y_ids = iota((lat, slots), 0).astype(F32)
    edges = weighted(
        jnp.concatenate(
            [
                jnp.where(y_ids == lat_row, last, 0.0).astype(BF16),
                jnp.where(lat_row == lat - 1.0, wx_f, 0.0).astype(BF16),
            ],
            axis=0,
        )
    )
    far_col = edges[0:lat, levels:]
    shifted = jnp.where(iota((lat, levels), 0) == 0, 0.0, pltpu.roll(far_col, 1, 0))
    col_send[...] = edges[0:lat, 0:levels] + shifted
    corner_send[...] = pltpu.roll(far_col, 1, 0)[0:PAD]
    row_send[...] = edges[lat:, levels:].astype(BF16)
    f_copies = [
        pltpu.make_async_remote_copy(
            src_ref=src, dst_ref=dst, send_sem=f_send.at[i], recv_sem=f_recv.at[i],
            device_id=device, device_id_type=MESH,
        )
        for i, (src, dst, device) in enumerate(
            (
                (col_send, col_recv, east),
                (row_send, row_recv, north),
                (corner_send, corner_recv, (gx_up, gy_up)),
            )
        )
    ]
    for copy in f_copies:
        copy.start()

    group = 4

    def force(i, carry):
        parts = []
        for j in range(group):
            hot = jnp.where(lat_row == (i * group + j).astype(F32), 1.0, 0.0).astype(BF16)
            parts.append(wx[...] * hot)
        total = weighted(jnp.concatenate(parts, axis=0))
        for j in range(group + 1):
            rows = pl.ds((i * group + j) * lon, lon)
            add = None
            if j < group:
                add = total[j * lon : (j + 1) * lon, 0:levels]
            if j:
                behind = total[(j - 1) * lon : j * lon, levels:]
                add = behind if add is None else add + behind
            st[rows, :] = st[rows, :] + add
        return carry

    lax.fori_loop(0, lat // group, force, 0)
    for copy in f_copies:
        copy.wait()
    first_x = iota((lon, levels), 0) == 0
    st[0:lon, :] = st[0:lon, :] + jnp.where(
        gy > 0, row_recv[...].astype(F32) + jnp.where(first_x, corner_recv[0:1, :], 0.0), 0.0
    )
    edge = pl.ds(0, lat, stride=lon)
    st[edge, :] = st[edge, :] + col_recv[...]

    def row_at(parity, y):
        return (parity * (lat + 2) + y + 1) * wide + PAD

    def x_copies(step, b):
        copies = []
        for side, device in ((0, west), (1, east)):
            copies.append(
                pltpu.make_async_remote_copy(
                    src_ref=xs.at[step % 2, side, pl.ds(b * ROWS, ROWS)],
                    dst_ref=xr.at[step, 1 - side, pl.ds(b * ROWS, ROWS)],
                    send_sem=x_send.at[step, side, b], recv_sem=x_recv.at[step, 1 - side, b],
                    device_id=device, device_id_type=MESH,
                )
            )
        return copies

    def y_copies(step):
        return [
            pltpu.make_async_remote_copy(
                src_ref=ys.at[step % 2, side], dst_ref=yr.at[step, 1 - side],
                send_sem=y_send.at[step, side], recv_sem=y_recv.at[step, 1 - side],
                device_id=device, device_id_type=MESH,
            )
            for side, device in ((0, south), (1, north))
        ]

    def edges_in(step, b):
        for copy in x_copies(step, b):
            copy.wait()
        base = row_at(step % 2, b * ROWS)
        fb[pl.ds(base - 1, ROWS, stride=wide), :] = xr[step, 0, pl.ds(b * ROWS, ROWS), :]
        fb[pl.ds(base + lon, ROWS, stride=wide), :] = xr[step, 1, pl.ds(b * ROWS, ROWS), :]

    def advanced(step, y):
        base = row_at(step % 2, y)
        total = fb[pl.ds(base - 1, lon), :] + fb[pl.ds(base + 1, lon), :]
        total = total + (fb[pl.ds(base - wide, lon), :] + fb[pl.ds(base + wide, lon), :])
        return st[pl.ds(y * lon, lon), :] + total

    def halo(step):
        for copy in y_copies(step):
            copy.wait()
        parity = step % 2
        fb[pl.ds(row_at(parity, -1), lon), :] = jnp.where(gy > 0, yr[step, 0].astype(F32), 0.0)
        fb[pl.ds(row_at(parity, lat), lon), :] = jnp.where(
            gy < n_gy - 1, yr[step, 1].astype(F32), 0.0
        )

    def order(i):
        return jnp.where(i == 0, 0, jnp.where(i == 1, blocks - 1, i - 1))

    def section(step, y):
        rows = pl.ds(y * lon, lon)
        lam = st[rows, :] if step == 0 else advanced(step - 1, y)
        pair = wst[y]
        product = jnp.dot(
            jnp.concatenate(split(lam), axis=1),
            jnp.concatenate([pair, pair], axis=0),
            preferred_element_type=F32,
        )
        mixed = product[:, 0:levels] + product[:, levels:]
        flux = df[rows, :] * mixed
        st[rows, :] = mixed - 4.0 * flux
        fb[pl.ds(row_at(step % 2, y), lon), :] = flux

    def block(step, i, carry):
        b = order(i)
        if step:
            edges_in(step - 1, b)
        for j in range(ROWS):
            section(step, b * ROWS + j)
        base = row_at(step % 2, b * ROWS)
        part = pl.ds(b * ROWS, ROWS)
        xs[step % 2, 0, part, :] = fb[pl.ds(base, ROWS, stride=wide), :]
        xs[step % 2, 1, part, :] = fb[pl.ds(base + lon - 1, ROWS, stride=wide), :]
        for copy in x_copies(step, b):
            copy.start()
        return carry

    for y in range(lat):
        rows = pl.ds(y * lon, lon)
        pltpu.make_async_copy(diff_hbm.at[:, y, :], df.at[rows], df_sem.at[y]).wait()
    for step in range(STEPS):
        if step:
            halo(step - 1)
        lax.fori_loop(0, 2, functools.partial(block, step), 0)
        ys[step % 2, 0] = fb[pl.ds(row_at(step % 2, 0), lon), :].astype(BF16)
        ys[step % 2, 1] = fb[pl.ds(row_at(step % 2, lat - 1), lon), :].astype(BF16)
        for copy in y_copies(step):
            copy.start()
        lax.fori_loop(2, blocks, functools.partial(block, step), 0)

    halo(STEPS - 1)

    def store(y):
        return pltpu.make_async_copy(
            obuf.at[pl.ds(y * lon, lon)], out_hbm.at[:, y, :], out_sem.at[y]
        )

    def finish(i, carry):
        b = order(i)
        edges_in(STEPS - 1, b)
        for j in range(ROWS):
            y = b * ROWS + j
            obuf[pl.ds(y * lon, lon), :] = advanced(STEPS - 1, y)
            store(y).start()
        return carry

    lax.fori_loop(0, blocks, finish, 0)

    def sent(k, carry):
        for copy in block_copies(k):
            copy.wait_send()
        return carry

    lax.fori_loop(1, n_all, sent, 0)

    def stored(y, carry):
        store(y).wait()
        return carry

    lax.fori_loop(0, lat, stored, 0)


def solution(mesh):
    n_gx, n_gy = mesh.shape["gx"], mesh.shape["gy"]

    def shards(state, diffusion, vert_inverse, profiles, counts, cell_lon, cell_lat, weight_slot):
        lon, lat, levels = state.shape
        n_all = counts.shape[1]
        slots = n_all * CAP
        blocks = lat // ROWS
        wide = lon + 2 * PAD
        dma = pltpu.SemaphoreType.DMA
        vmem = pl.BlockSpec(memory_space=pltpu.VMEM)
        out = pl.pallas_call(
            functools.partial(kernel, n_gx, n_gy),
            out_shape=jax.ShapeDtypeStruct((lon, lat, levels), F32),
            in_specs=[vmem] * 5 + [pl.BlockSpec(memory_space=pl.ANY)] * 3,
            out_specs=pl.BlockSpec(memory_space=pl.ANY),
            scratch_shapes=[
                pltpu.VMEM(((lat + 1) * lon, levels), F32),
                pltpu.VMEM((lat * lon, levels), F32),
                pltpu.VMEM((lat, levels, levels), F32),
                pltpu.VMEM((lat, levels, 2 * levels), BF16),
                pltpu.VMEM((2 * (lat + 2) * wide, levels), F32),
                pltpu.VMEM((lat * lon, levels), F32),
                pltpu.VMEM((n_all, CAP, levels), BF16),
                pltpu.VMEM((n_all, 1, levels), F32),
                pltpu.VMEM((n_all, CAP, levels), BF16),
                pltpu.VMEM((n_all, 1, levels), F32),
                pltpu.VMEM((lon, slots), BF16),
                pltpu.VMEM((slots, 2 * levels), BF16),
                pltpu.VMEM((slots, 2 * levels), BF16),
                pltpu.VMEM((lat, levels), F32),
                pltpu.VMEM((lat, levels), F32),
                pltpu.VMEM((lon, levels), BF16),
                pltpu.VMEM((lon, levels), BF16),
                pltpu.VMEM((PAD, levels), F32),
                pltpu.VMEM((PAD, levels), F32),
                pltpu.VMEM((2, 2, lat, levels), F32),
                pltpu.VMEM((STEPS, 2, lat, levels), F32),
                pltpu.VMEM((2, 2, lon, levels), BF16),
                pltpu.VMEM((STEPS, 2, lon, levels), BF16),
                dma((blocks,)), dma((lat,)), dma((lat,)), dma((lat,)),
                dma((n_all,)), dma((n_all,)), dma((n_all,)), dma((n_all,)),
                dma((3,)), dma((3,)),
                dma((STEPS, 2, blocks)), dma((STEPS, 2, blocks)),
                dma((STEPS, 2)), dma((STEPS, 2)),
            ],
            compiler_params=pltpu.CompilerParams(
                collective_id=0, has_side_effects=True, vmem_limit_bytes=VMEM_LIMIT
            ),
            name="adjoint",
        )(
            profiles, counts, cell_lon[None], cell_lat[None], weight_slot,
            state, diffusion, vert_inverse,
        )
        return out

    return jax.shard_map(
        shards,
        mesh=mesh,
        in_specs=(
            P("gx", "gy", None),
            P("gx", "gy", None),
            P("gy", None, None),
            P(("gx", "gy"), None),
            P(("gx", "gy"), None),
            P(("gx", "gy")),
            P(("gx", "gy")),
            P(None, ("gx", "gy")),
        ),
        out_specs=P("gx", "gy", None),
        check_vma=False,
    )
```

```python
import functools

import jax
import jax.numpy as jnp
from jax import lax
from jax.experimental import pallas as pl
from jax.experimental.pallas import tpu as pltpu
from jax.sharding import PartitionSpec as P

CAP = 16
STEPS = 4
SLOTS = 64
PAD = 8
ROWS = 8
HALF = ROWS // 2
FIELDS = 4
F32 = jnp.float32
BF16 = jnp.bfloat16
MESH = pl.DeviceIdType.MESH
VMEM_LIMIT = 48 * 1024 * 1024


def split(value):
    upper = value.astype(BF16)
    return upper, (value - upper.astype(F32)).astype(BF16)


def iota(shape, axis):
    return lax.broadcasted_iota(jnp.int32, shape, axis)


def kernel(
    n_gx, n_gy,
    prof_hbm, counts_hbm, lon_hbm, lat_hbm, slot_hbm, state_hbm, diff_hbm, inv_hbm, obuf,
    prof_ref, counts_ref, lon_ref, lat_ref, slot_ref, st, df, wf, wst, fb, msg, mmsg, recv, mrecv, wx, upper, lower,
    col_send, col_recv, near_row, row_send, row_recv, corner_send, corner_recv,
    xs, xr, ys, yr,
    small_sem, w_sem, st_sem, df_sem, v_send, v_recv, m_send, m_recv,
    f_send, f_recv, x_send, x_recv, y_send, y_recv,
):
    lon, lat, levels = state_hbm.shape
    n_all = n_gx * n_gy
    slots = n_all * CAP
    obs = prof_ref.shape[0]
    blocks = lat // ROWS
    wide = lon + 2 * PAD
    gx, gy = lax.axis_index("gx"), lax.axis_index("gy")
    me = gx * n_gy + gy
    gx_up, gx_down = lax.rem(gx + 1, n_gx), lax.rem(gx + n_gx - 1, n_gx)
    gy_up, gy_down = lax.rem(gy + 1, n_gy), lax.rem(gy + n_gy - 1, n_gy)
    east, west, north, south = (gx_up, gy), (gx_down, gy), (gx, gy_up), (gx, gy_down)

    small_loads = [
        pltpu.make_async_copy(src, dst, small_sem.at[i])
        for i, (src, dst) in enumerate(
            (
                (counts_hbm, counts_ref), (prof_hbm, prof_ref), (lon_hbm, lon_ref),
                (lat_hbm, lat_ref), (slot_hbm, slot_ref),
            )
        )
    ]
    for load in small_loads:
        load.start()

    columns = [lax.rem(gx + d, n_gx) for d in range(n_gx)]
    lines = [lax.rem(gy + d, n_gy) for d in range(n_gy)]
    peers = [(column, line) for column in columns for line in lines]

    barrier = pltpu.get_barrier_semaphore()
    for peer in peers[1:]:
        pl.semaphore_signal(barrier, inc=1, device_id=peer, device_id_type=MESH)

    w_loads = [
        pltpu.make_async_copy(
            inv_hbm.at[pl.ds(b * ROWS, ROWS)], wf.at[pl.ds(b * ROWS, ROWS)], w_sem.at[b]
        )
        for b in range(blocks)
    ]
    for load in w_loads:
        load.start()
    for y in range(lat):
        rows = pl.ds(y * lon, lon)
        pltpu.make_async_copy(state_hbm.at[:, y, :], st.at[rows], st_sem.at[y]).start()
    for y in range(lat):
        rows = pl.ds(y * lon, lon)
        pltpu.make_async_copy(diff_hbm.at[:, y, :], df.at[rows], df_sem.at[y]).start()

    for load in small_loads:
        load.wait()

    count_row = counts_ref[...].astype(F32)
    dest, lane = iota((n_all, n_all), 0), iota((n_all, n_all), 1)
    start = jnp.sum(jnp.where(lane < dest, count_row, 0.0), axis=1, keepdims=True)
    count = jnp.sum(jnp.where(lane == dest, count_row, 0.0), axis=1, keepdims=True)
    position = iota((n_all, obs), 1).astype(F32)
    inside = jnp.where((position >= start) & (position < start + count), 1.0, 0.0)
    owner = iota((n_all, obs), 0).astype(F32)
    slot_of = jnp.sum(inside * (position - start), axis=0, keepdims=True)
    code = jnp.sum(inside * owner, axis=0, keepdims=True) * CAP + slot_of
    selector = jnp.where(iota((slots, obs), 0) == code.astype(jnp.int32), 1.0, 0.0).astype(BF16)
    msg[...] = (
        jnp.dot(selector, prof_ref[...], preferred_element_type=F32)
        .astype(BF16)
        .reshape(n_all, CAP, levels)
    )
    field = iota((levels, obs), 0)
    meta = jnp.where(field < CAP, lon_ref[...].astype(F32), lat_ref[...].astype(F32))
    meta = jnp.where(field < 2 * CAP, meta, slot_ref[0:1, :].astype(F32))
    meta = jnp.where(field < 3 * CAP, meta, slot_ref[1:2, :].astype(F32))
    meta = jnp.where(field % CAP == slot_of.astype(jnp.int32), meta, 0.0).astype(BF16)
    mmsg[...] = lax.dot_general(
        inside.astype(BF16), meta, (((1,), (1,)), ((), ())), preferred_element_type=F32
    ).reshape(n_all, 1, levels)

    pl.semaphore_wait(barrier, n_all - 1)

    sends = []
    for k, (column, line) in enumerate(peers[1:], 1):
        other = column * n_gy + line
        for src, dst, send_sem, recv_sem in (
            (msg, recv, v_send, v_recv), (mmsg, mrecv, m_send, m_recv)
        ):
            sends.append(
                pltpu.make_async_remote_copy(
                    src_ref=src.at[other], dst_ref=dst.at[k],
                    send_sem=send_sem.at[k], recv_sem=recv_sem.at[k],
                    device_id=(column, line), device_id_type=MESH,
                )
            )
    for copy in sends:
        copy.start()
    recv[0] = msg[me]
    mrecv[0] = mmsg[me]

    for b in range(blocks):
        w_loads[b].wait()

        def pairs(i, carry):
            for j in range(2):
                y = b * ROWS + 2 * i + j
                wst[y] = jnp.concatenate(split(wf[y]), axis=1)
            return carry

        lax.fori_loop(0, ROWS // 2, pairs, 0)

    for y in range(lat):
        rows = pl.ds(y * lon, lon)
        pltpu.make_async_copy(state_hbm.at[:, y, :], st.at[rows], st_sem.at[y]).wait()

    for copy in sends:
        copy.wait_recv()

    table = mrecv[...].reshape(n_all, levels)
    spread = jnp.where(iota((n_all, slots), 1) // CAP == iota((n_all, slots), 0), 1.0, 0.0)
    wide_table = lax.dot_general(
        table.astype(BF16), spread.astype(BF16), (((0,), (0,)), ((), ())),
        preferred_element_type=F32,
    )
    own = iota((levels, slots), 0) % CAP == iota((levels, slots), 1) % CAP
    wide_table = jnp.where(own, wide_table, 0.0)
    lon_row, lat_row, frac_row = [
        jnp.sum(wide_table[f * CAP : (f + 1) * CAP], axis=0, keepdims=True) for f in range(3)
    ]
    frac_row = frac_row / SLOTS
    x_ids = iota((lon, slots), 0).astype(F32)
    wx_f = jnp.where(x_ids == lon_row, 1.0 - frac_row, 0.0) + jnp.where(
        x_ids == lon_row + 1.0, frac_row, 0.0
    )
    wx[...] = wx_f.astype(BF16)
    pick = iota((CAP, levels), 1) - 3 * CAP == iota((CAP, levels), 0)

    for k in range(n_all):
        here = slice(k * CAP, (k + 1) * CAP)
        frac_y = (
            jnp.sum(jnp.where(pick, mrecv[k], 0.0), axis=1, keepdims=True) / SLOTS
        )
        values = recv[k].astype(F32)
        far = values * frac_y
        near_terms, far_terms = split(values - far), split(far)
        upper[here, 0:levels], lower[here, 0:levels] = near_terms
        upper[here, levels:], lower[here, levels:] = far_terms

    def weighted(rows):
        return jnp.dot(rows, upper[...], preferred_element_type=F32) + jnp.dot(
            rows, lower[...], preferred_element_type=F32
        )

    last = jnp.where(lon_row == lon - 1.0, frac_row, 0.0)
    y_ids = iota((lat, slots), 0).astype(F32)
    edges = weighted(
        jnp.concatenate(
            [
                jnp.where(y_ids == lat_row, last, 0.0).astype(BF16),
                jnp.where(lat_row == lat - 1.0, wx_f, 0.0).astype(BF16),
            ],
            axis=0,
        )
    )
    far_col = edges[0:lat, levels:]
    shifted = jnp.where(iota((lat, levels), 0) == 0, 0.0, pltpu.roll(far_col, 1, 0))
    col_send[...] = edges[0:lat, 0:levels] + shifted
    corner_send[...] = pltpu.roll(far_col, 1, 0)[0:PAD]
    row_send[...] = edges[lat:, levels:].astype(BF16)
    near_row[...] = edges[lat:, 0:levels]
    f_copies = [
        pltpu.make_async_remote_copy(
            src_ref=src, dst_ref=dst, send_sem=f_send.at[i], recv_sem=f_recv.at[i],
            device_id=device, device_id_type=MESH,
        )
        for i, (src, dst, device) in enumerate(
            (
                (col_send, col_recv, east),
                (row_send, row_recv, north),
                (corner_send, corner_recv, (gx_up, gy_up)),
            )
        )
    ]
    for copy in f_copies:
        copy.start()

    done_row = lat - HALF - 1

    def force(runs, edge):
        parts = []
        for low, size in runs:
            for j in range(size):
                y = low + j
                if not edge:
                    y = jnp.where(y == done_row, -1, y).astype(F32)
                hot = jnp.where(lat_row == y, 1.0, 0.0).astype(BF16)
                parts.append(wx[...] * hot)
        total = weighted(jnp.concatenate(parts, axis=0))
        at = 0
        for low, size in runs:
            for j in range(size + 1):
                rows = pl.ds((low + j) * lon, lon)
                add = None
                if j < size:
                    add = total[at * lon : (at + 1) * lon, 0:levels]
                if j:
                    behind = total[(at - 1) * lon : at * lon, levels:]
                    add = behind if add is None else add + behind
                st[rows, :] = st[rows, :] + add
                at = at + 1 if j < size else at

    def force_block(b, carry):
        force([(HALF + (b - 1) * ROWS, ROWS)], False)
        return carry

    force([(0, HALF), (done_row, HALF)], True)
    final = pl.ds((lat - 1) * lon, lon)
    st[final, :] = st[final, :] + near_row[...]
    early = blocks // 2 + 1
    lax.fori_loop(1, early, force_block, 0)
    for copy in f_copies:
        copy.wait()
    first_x = iota((lon, levels), 0) == 0
    st[0:lon, :] = st[0:lon, :] + jnp.where(
        gy > 0, row_recv[...].astype(F32) + jnp.where(first_x, corner_recv[0:1, :], 0.0), 0.0
    )
    edge = pl.ds(0, lat, stride=lon)
    st[edge, :] = st[edge, :] + col_recv[...]

    def row_at(parity, y):
        return (parity * (lat + 2) + y + 1) * wide + PAD

    def x_copies(step, b):
        copies = []
        for side, device in ((0, west), (1, east)):
            copies.append(
                pltpu.make_async_remote_copy(
                    src_ref=xs.at[step % 2, side, pl.ds(b * ROWS, ROWS)],
                    dst_ref=xr.at[step, 1 - side, pl.ds(b * ROWS, ROWS)],
                    send_sem=x_send.at[step, side, b], recv_sem=x_recv.at[step, 1 - side, b],
                    device_id=device, device_id_type=MESH,
                )
            )
        return copies

    def y_copies(step):
        return [
            pltpu.make_async_remote_copy(
                src_ref=ys.at[step % 2, side], dst_ref=yr.at[step, 1 - side],
                send_sem=y_send.at[step, side], recv_sem=y_recv.at[step, 1 - side],
                device_id=device, device_id_type=MESH,
            )
            for side, device in ((0, south), (1, north))
        ]

    def segments(b, edge):
        if edge:
            return [(0, HALF, 0), (lat - HALF, HALF, HALF)]
        return [(HALF + (b - 1) * ROWS, ROWS, b * ROWS)]

    def edges_in(step, b, edge):
        for copy in x_copies(step, b):
            copy.wait()
        for low, size, at in segments(b, edge):
            base = row_at(step % 2, low)
            part = pl.ds(at, size)
            fb[pl.ds(base - 1, size, stride=wide), :] = xr[step, 0, part, :]
            fb[pl.ds(base + lon, size, stride=wide), :] = xr[step, 1, part, :]

    def advanced(step, y):
        base = row_at(step % 2, y)
        total = fb[pl.ds(base - 1, lon), :] + fb[pl.ds(base + 1, lon), :]
        total = total + (fb[pl.ds(base - wide, lon), :] + fb[pl.ds(base + wide, lon), :])
        return st[pl.ds(y * lon, lon), :] + total

    def halo(step):
        for copy in y_copies(step):
            copy.wait()
        parity = step % 2
        fb[pl.ds(row_at(parity, -1), lon), :] = jnp.where(gy > 0, yr[step, 0].astype(F32), 0.0)
        fb[pl.ds(row_at(parity, lat), lon), :] = jnp.where(
            gy < n_gy - 1, yr[step, 1].astype(F32), 0.0
        )

    def section(step, y):
        rows = pl.ds(y * lon, lon)
        lam = st[rows, :] if step == 0 else advanced(step - 1, y)
        pair = wst[y]
        product = jnp.dot(
            jnp.concatenate(split(lam), axis=1),
            jnp.concatenate([pair, pair], axis=0),
            preferred_element_type=F32,
        )
        mixed = product[:, 0:levels] + product[:, levels:]
        flux = df[rows, :] * mixed
        st[rows, :] = mixed - 4.0 * flux
        fb[pl.ds(row_at(step % 2, y), lon), :] = flux

    def block(step, b, edge):
        if step:
            edges_in(step - 1, b, edge)
        for low, size, _ in segments(b, edge):
            for j in range(size):
                section(step, low + j)
        for low, size, at in segments(b, edge):
            base = row_at(step % 2, low)
            part = pl.ds(at, size)
            xs[step % 2, 0, part, :] = fb[pl.ds(base, size, stride=wide), :]
            xs[step % 2, 1, part, :] = fb[pl.ds(base + lon - 1, size, stride=wide), :]
        for copy in x_copies(step, b):
            copy.start()

    def edge_block(step):
        if step:
            halo(step - 1)
        block(step, 0, True)
        ys[step % 2, 0] = fb[pl.ds(row_at(step % 2, 0), lon), :].astype(BF16)
        ys[step % 2, 1] = fb[pl.ds(row_at(step % 2, lat - 1), lon), :].astype(BF16)
        for copy in y_copies(step):
            copy.start()

    def inner_blocks(step, low, high):
        def one(b, carry):
            block(step, b, False)
            return carry

        lax.fori_loop(low, high, one, 0)

    def finish(b, edge):
        edges_in(STEPS - 1, b, edge)
        for low, size, _ in segments(b, edge):
            for j in range(size):
                obuf[pl.ds((low + j) * lon, lon), :] = advanced(STEPS - 1, low + j)

    def finish_inner(b, carry):
        finish(b, False)
        return carry

    for y in range(lat):
        rows = pl.ds(y * lon, lon)
        pltpu.make_async_copy(diff_hbm.at[:, y, :], df.at[rows], df_sem.at[y]).wait()
    edge_block(0)
    lax.fori_loop(early, blocks, force_block, 0)
    inner_blocks(0, 1, blocks)
    edge_block(1)
    inner_blocks(1, 1, blocks)
    inner_blocks(2, 1, early)
    edge_block(2)
    inner_blocks(2, early, blocks)
    inner_blocks(3, 1, blocks)
    edge_block(3)
    lax.fori_loop(1, blocks, finish_inner, 0)
    halo(STEPS - 1)
    finish(0, True)
    for copy in sends:
        copy.wait_send()


def store_kernel(rows_ref, out_hbm, sem):
    lon, lat, _ = out_hbm.shape

    def store(y):
        return pltpu.make_async_copy(
            rows_ref.at[pl.ds(y * lon, lon)], out_hbm.at[:, y, :], sem.at[y]
        )

    for y in range(lat):
        store(y).start()
    for y in range(lat):
        store(y).wait()


def solution(mesh):
    n_gx, n_gy = mesh.shape["gx"], mesh.shape["gy"]

    def shards(state, diffusion, vert_inverse, profiles, counts, cell_lon, cell_lat, weight_slot):
        lon, lat, levels = state.shape
        n_all = counts.shape[1]
        slots = n_all * CAP
        blocks = lat // ROWS
        wide = lon + 2 * PAD
        dma = pltpu.SemaphoreType.DMA
        vmem = pl.BlockSpec(memory_space=pltpu.VMEM)
        obs = profiles.shape[0]
        out = pl.pallas_call(
            functools.partial(kernel, n_gx, n_gy),
            out_shape=pltpu.VMEM((lat * lon, levels), F32),
            in_specs=[pl.BlockSpec(memory_space=pltpu.HBM)] * 8,
            out_specs=vmem,
            scratch_shapes=[
                pltpu.VMEM((obs, levels), BF16),
                pltpu.VMEM((1, n_all), jnp.int32),
                pltpu.VMEM((1, obs), jnp.int32),
                pltpu.VMEM((1, obs), jnp.int32),
                pltpu.VMEM((2, obs), jnp.int32),
                pltpu.VMEM((lat * lon, levels), F32),
                pltpu.VMEM((lat * lon, levels), F32),
                pltpu.VMEM((lat, levels, levels), F32),
                pltpu.VMEM((lat, levels, 2 * levels), BF16),
                pltpu.VMEM((2 * (lat + 2) * wide, levels), F32),
                pltpu.VMEM((n_all, CAP, levels), BF16),
                pltpu.VMEM((n_all, 1, levels), F32),
                pltpu.VMEM((n_all, CAP, levels), BF16),
                pltpu.VMEM((n_all, 1, levels), F32),
                pltpu.VMEM((lon, slots), BF16),
                pltpu.VMEM((slots, 2 * levels), BF16),
                pltpu.VMEM((slots, 2 * levels), BF16),
                pltpu.VMEM((lat, levels), F32),
                pltpu.VMEM((lat, levels), F32),
                pltpu.VMEM((lon, levels), F32),
                pltpu.VMEM((lon, levels), BF16),
                pltpu.VMEM((lon, levels), BF16),
                pltpu.VMEM((PAD, levels), F32),
                pltpu.VMEM((PAD, levels), F32),
                pltpu.VMEM((2, 2, lat, levels), F32),
                pltpu.VMEM((STEPS, 2, lat, levels), F32),
                pltpu.VMEM((2, 2, lon, levels), BF16),
                pltpu.VMEM((STEPS, 2, lon, levels), BF16),
                dma((5,)), dma((blocks,)), dma((lat,)), dma((lat,)),
                dma((n_all,)), dma((n_all,)), dma((n_all,)), dma((n_all,)),
                dma((3,)), dma((3,)),
                dma((STEPS, 2, blocks)), dma((STEPS, 2, blocks)),
                dma((STEPS, 2)), dma((STEPS, 2)),
            ],
            compiler_params=pltpu.CompilerParams(
                collective_id=0, has_side_effects=True, vmem_limit_bytes=VMEM_LIMIT
            ),
            name="adjoint",
        )(
            *[
                pltpu.with_memory_space_constraint(x, pltpu.HBM)
                for x in (
                    profiles, counts, cell_lon[None], cell_lat[None], weight_slot,
                    state, diffusion, vert_inverse,
                )
            ]
        )
        return pl.pallas_call(
            store_kernel,
            out_shape=jax.ShapeDtypeStruct((lon, lat, levels), F32),
            in_specs=[vmem],
            out_specs=pl.BlockSpec(memory_space=pl.ANY),
            scratch_shapes=[dma((lat,))],
            compiler_params=pltpu.CompilerParams(vmem_limit_bytes=8 * 1024 * 1024),
            name="store",
        )(pltpu.with_memory_space_constraint(out, pltpu.VMEM))

    return jax.shard_map(
        shards,
        mesh=mesh,
        in_specs=(
            P("gx", "gy", None),
            P("gx", "gy", None),
            P("gy", None, None),
            P(("gx", "gy"), None),
            P(("gx", "gy"), None),
            P(("gx", "gy")),
            P(("gx", "gy")),
            P(None, ("gx", "gy")),
        ),
        out_specs=P("gx", "gy", None),
        check_vma=False,
    )
```

```python
import functools

import jax
import jax.numpy as jnp
from jax import lax
from jax.experimental import pallas as pl
from jax.experimental.pallas import tpu as pltpu
from jax.sharding import PartitionSpec as P

CAP = 16
STEPS = 4
SLOTS = 64
PAD = 8
ROWS = 8
HALF = ROWS // 2
FIELDS = 4
F32 = jnp.float32
BF16 = jnp.bfloat16
MESH = pl.DeviceIdType.MESH
VMEM_LIMIT = 48 * 1024 * 1024


def split(value):
    upper = value.astype(BF16)
    return upper, (value - upper.astype(F32)).astype(BF16)


def iota(shape, axis):
    return lax.broadcasted_iota(jnp.int32, shape, axis)


def kernel(
    n_gx, n_gy,
    prof_hbm, counts_hbm, lon_hbm, lat_hbm, slot_hbm, state_hbm, diff_hbm, inv_hbm, obuf,
    prof_ref, counts_ref, lon_ref, lat_ref, slot_ref, st, df, wf, wst, fb, msg, mmsg, recv, mrecv, wx, upper, lower,
    col_send, col_recv, near_row, row_send, row_recv, corner_send, corner_recv,
    xs, xr, ys, yr,
    small_sem, w_sem, st_sem, df_sem, v_send, v_recv, m_send, m_recv,
    f_send, f_recv, x_send, x_recv, y_send, y_recv,
):
    lon, lat, levels = state_hbm.shape
    n_all = n_gx * n_gy
    slots = n_all * CAP
    obs = prof_ref.shape[0]
    blocks = lat // ROWS
    wide = lon + 2 * PAD
    gx, gy = lax.axis_index("gx"), lax.axis_index("gy")
    me = gx * n_gy + gy
    gx_up, gx_down = lax.rem(gx + 1, n_gx), lax.rem(gx + n_gx - 1, n_gx)
    gy_up, gy_down = lax.rem(gy + 1, n_gy), lax.rem(gy + n_gy - 1, n_gy)
    east, west, north, south = (gx_up, gy), (gx_down, gy), (gx, gy_up), (gx, gy_down)

    small_loads = [
        pltpu.make_async_copy(src, dst, small_sem.at[i])
        for i, (src, dst) in enumerate(
            (
                (counts_hbm, counts_ref), (prof_hbm, prof_ref), (lon_hbm, lon_ref),
                (lat_hbm, lat_ref), (slot_hbm, slot_ref),
            )
        )
    ]
    for load in small_loads:
        load.start()

    columns = [lax.rem(gx + d, n_gx) for d in range(n_gx)]
    lines = [lax.rem(gy + d, n_gy) for d in range(n_gy)]
    peers = [(column, line) for column in columns for line in lines]

    barrier = pltpu.get_barrier_semaphore()
    for peer in peers[1:]:
        pl.semaphore_signal(barrier, inc=1, device_id=peer, device_id_type=MESH)

    for load in small_loads:
        load.wait()

    w_loads = [
        pltpu.make_async_copy(
            inv_hbm.at[pl.ds(b * ROWS, ROWS)], wf.at[pl.ds(b * ROWS, ROWS)], w_sem.at[b]
        )
        for b in range(blocks)
    ]
    for load in w_loads:
        load.start()
    for y in range(lat):
        rows = pl.ds(y * lon, lon)
        pltpu.make_async_copy(state_hbm.at[:, y, :], st.at[rows], st_sem.at[y]).start()
    for y in range(lat):
        rows = pl.ds(y * lon, lon)
        pltpu.make_async_copy(diff_hbm.at[:, y, :], df.at[rows], df_sem.at[y]).start()

    count_row = counts_ref[...].astype(F32)
    dest, lane = iota((n_all, n_all), 0), iota((n_all, n_all), 1)
    start = jnp.sum(jnp.where(lane < dest, count_row, 0.0), axis=1, keepdims=True)
    count = jnp.sum(jnp.where(lane == dest, count_row, 0.0), axis=1, keepdims=True)
    position = iota((n_all, obs), 1).astype(F32)
    inside = jnp.where((position >= start) & (position < start + count), 1.0, 0.0)
    owner = iota((n_all, obs), 0).astype(F32)
    slot_of = jnp.sum(inside * (position - start), axis=0, keepdims=True)
    code = jnp.sum(inside * owner, axis=0, keepdims=True) * CAP + slot_of
    selector = jnp.where(iota((slots, obs), 0) == code.astype(jnp.int32), 1.0, 0.0).astype(BF16)
    msg[...] = (
        jnp.dot(selector, prof_ref[...], preferred_element_type=F32)
        .astype(BF16)
        .reshape(n_all, CAP, levels)
    )
    field = iota((levels, obs), 0)
    meta = jnp.where(field < CAP, lon_ref[...].astype(F32), lat_ref[...].astype(F32))
    meta = jnp.where(field < 2 * CAP, meta, slot_ref[0:1, :].astype(F32))
    meta = jnp.where(field < 3 * CAP, meta, slot_ref[1:2, :].astype(F32))
    meta = jnp.where(field % CAP == slot_of.astype(jnp.int32), meta, 0.0).astype(BF16)
    mmsg[...] = lax.dot_general(
        inside.astype(BF16), meta, (((1,), (1,)), ((), ())), preferred_element_type=F32
    ).reshape(n_all, 1, levels)

    pl.semaphore_wait(barrier, n_all - 1)

    sends = []
    for k, (column, line) in enumerate(peers[1:], 1):
        other = column * n_gy + line
        for src, dst, send_sem, recv_sem in (
            (msg, recv, v_send, v_recv), (mmsg, mrecv, m_send, m_recv)
        ):
            sends.append(
                pltpu.make_async_remote_copy(
                    src_ref=src.at[other], dst_ref=dst.at[k],
                    send_sem=send_sem.at[k], recv_sem=recv_sem.at[k],
                    device_id=(column, line), device_id_type=MESH,
                )
            )
    for copy in sends:
        copy.start()
    recv[0] = msg[me]
    mrecv[0] = mmsg[me]

    for b in range(blocks):
        w_loads[b].wait()

        def pairs(i, carry):
            for j in range(2):
                y = b * ROWS + 2 * i + j
                wst[y] = jnp.concatenate(split(wf[y]), axis=1)
            return carry

        lax.fori_loop(0, ROWS // 2, pairs, 0)

    for y in range(lat):
        rows = pl.ds(y * lon, lon)
        pltpu.make_async_copy(state_hbm.at[:, y, :], st.at[rows], st_sem.at[y]).wait()

    for y in range(lat):
        rows = pl.ds(y * lon, lon)
        pltpu.make_async_copy(diff_hbm.at[:, y, :], df.at[rows], df_sem.at[y]).wait()

    pick = iota((CAP, levels), 1) - 3 * CAP == iota((CAP, levels), 0)
    batch = n_all
    for k in range(n_all):
        if k % batch == 0:
            for copy in sends[max(2 * k - 2, 0) : 2 * (k + batch) - 2]:
                copy.wait_recv()
        here = slice(k * CAP, (k + 1) * CAP)
        frac_y = (
            jnp.sum(jnp.where(pick, mrecv[k], 0.0), axis=1, keepdims=True) / SLOTS
        )
        values = recv[k].astype(F32)
        far = values * frac_y
        near_terms, far_terms = split(values - far), split(far)
        upper[here, 0:levels], lower[here, 0:levels] = near_terms
        upper[here, levels:], lower[here, levels:] = far_terms

    table = mrecv[...].reshape(n_all, levels)
    spread = jnp.where(iota((n_all, slots), 1) // CAP == iota((n_all, slots), 0), 1.0, 0.0)
    wide_table = lax.dot_general(
        table.astype(BF16), spread.astype(BF16), (((0,), (0,)), ((), ())),
        preferred_element_type=F32,
    )
    own = iota((levels, slots), 0) % CAP == iota((levels, slots), 1) % CAP
    wide_table = jnp.where(own, wide_table, 0.0)
    lon_row, lat_row, frac_row = [
        jnp.sum(wide_table[f * CAP : (f + 1) * CAP], axis=0, keepdims=True) for f in range(3)
    ]
    frac_row = frac_row / SLOTS
    x_ids = iota((lon, slots), 0).astype(F32)
    wx_f = jnp.where(x_ids == lon_row, 1.0 - frac_row, 0.0) + jnp.where(
        x_ids == lon_row + 1.0, frac_row, 0.0
    )
    wx[...] = wx_f.astype(BF16)
    def weighted(rows):
        return jnp.dot(rows, upper[...], preferred_element_type=F32) + jnp.dot(
            rows, lower[...], preferred_element_type=F32
        )

    last = jnp.where(lon_row == lon - 1.0, frac_row, 0.0)
    y_ids = iota((lat, slots), 0).astype(F32)
    edges = weighted(
        jnp.concatenate(
            [
                jnp.where(y_ids == lat_row, last, 0.0).astype(BF16),
                jnp.where(lat_row == lat - 1.0, wx_f, 0.0).astype(BF16),
            ],
            axis=0,
        )
    )
    far_col = edges[0:lat, levels:]
    shifted = jnp.where(iota((lat, levels), 0) == 0, 0.0, pltpu.roll(far_col, 1, 0))
    col_send[...] = edges[0:lat, 0:levels] + shifted
    corner_send[...] = pltpu.roll(far_col, 1, 0)[0:PAD]
    row_send[...] = edges[lat:, levels:].astype(BF16)
    near_row[...] = edges[lat:, 0:levels]
    f_copies = [
        pltpu.make_async_remote_copy(
            src_ref=src, dst_ref=dst, send_sem=f_send.at[i], recv_sem=f_recv.at[i],
            device_id=device, device_id_type=MESH,
        )
        for i, (src, dst, device) in enumerate(
            (
                (col_send, col_recv, east),
                (row_send, row_recv, north),
                (corner_send, corner_recv, (gx_up, gy_up)),
            )
        )
    ]
    for copy in f_copies:
        copy.start()

    done_row = lat - HALF - 1

    def force(runs, edge):
        parts = []
        for low, size in runs:
            for j in range(size):
                y = low + j
                if not edge:
                    y = jnp.where(y == done_row, -1, y).astype(F32)
                hot = jnp.where(lat_row == y, 1.0, 0.0).astype(BF16)
                parts.append(wx[...] * hot)
        total = weighted(jnp.concatenate(parts, axis=0))
        at = 0
        for low, size in runs:
            for j in range(size + 1):
                rows = pl.ds((low + j) * lon, lon)
                add = None
                if j < size:
                    add = total[at * lon : (at + 1) * lon, 0:levels]
                if j:
                    behind = total[(at - 1) * lon : at * lon, levels:]
                    add = behind if add is None else add + behind
                st[rows, :] = st[rows, :] + add
                at = at + 1 if j < size else at

    def force_block(b, carry):
        force([(HALF + (b - 1) * ROWS, ROWS)], False)
        return carry

    force([(0, HALF), (done_row, HALF)], True)
    final = pl.ds((lat - 1) * lon, lon)
    st[final, :] = st[final, :] + near_row[...]
    early = (3 * blocks) // 4
    middle = (3 * blocks) // 4
    lax.fori_loop(1, early, force_block, 0)
    for copy in f_copies:
        copy.wait()
    first_x = iota((lon, levels), 0) == 0

    def add_column(y):
        rows = pl.ds(y * lon, lon)
        st[rows, :] = st[rows, :] + jnp.where(first_x, col_recv[y : y + 1, :], 0.0)

    def add_columns():
        y = iota((lat, levels), 0)
        edge = pl.ds(0, lat, stride=lon)
        st[edge, :] = st[edge, :] + jnp.where((y > 0) & (y < lat - 1), col_recv[...], 0.0)

    st[0:lon, :] = st[0:lon, :] + jnp.where(
        gy > 0, row_recv[...].astype(F32) + jnp.where(first_x, corner_recv[0:1, :], 0.0), 0.0
    )
    add_column(0)
    add_column(lat - 1)

    def row_at(parity, y):
        return (parity * (lat + 2) + y + 1) * wide + PAD

    def x_copies(step, b):
        copies = []
        for side, device in ((0, west), (1, east)):
            copies.append(
                pltpu.make_async_remote_copy(
                    src_ref=xs.at[step % 2, side, pl.ds(b * ROWS, ROWS)],
                    dst_ref=xr.at[step, 1 - side, pl.ds(b * ROWS, ROWS)],
                    send_sem=x_send.at[step, side, b], recv_sem=x_recv.at[step, 1 - side, b],
                    device_id=device, device_id_type=MESH,
                )
            )
        return copies

    def y_copies(step):
        return [
            pltpu.make_async_remote_copy(
                src_ref=ys.at[step % 2, side], dst_ref=yr.at[step, 1 - side],
                send_sem=y_send.at[step, side], recv_sem=y_recv.at[step, 1 - side],
                device_id=device, device_id_type=MESH,
            )
            for side, device in ((0, south), (1, north))
        ]

    def segments(b, edge):
        if edge:
            return [(0, HALF, 0), (lat - HALF, HALF, HALF)]
        return [(HALF + (b - 1) * ROWS, ROWS, b * ROWS)]

    def edges_in(step, b, edge):
        for copy in x_copies(step, b):
            copy.wait()
        for low, size, at in segments(b, edge):
            base = row_at(step % 2, low)
            part = pl.ds(at, size)
            fb[pl.ds(base - 1, size, stride=wide), :] = xr[step, 0, part, :]
            fb[pl.ds(base + lon, size, stride=wide), :] = xr[step, 1, part, :]

    def advanced(step, y):
        base = row_at(step % 2, y)
        total = fb[pl.ds(base - 1, lon), :] + fb[pl.ds(base + 1, lon), :]
        total = total + (fb[pl.ds(base - wide, lon), :] + fb[pl.ds(base + wide, lon), :])
        return st[pl.ds(y * lon, lon), :] + total

    def halo(step):
        for copy in y_copies(step):
            copy.wait()
        parity = step % 2
        fb[pl.ds(row_at(parity, -1), lon), :] = jnp.where(gy > 0, yr[step, 0].astype(F32), 0.0)
        fb[pl.ds(row_at(parity, lat), lon), :] = jnp.where(
            gy < n_gy - 1, yr[step, 1].astype(F32), 0.0
        )

    def section(step, y):
        rows = pl.ds(y * lon, lon)
        lam = st[rows, :] if step == 0 else advanced(step - 1, y)
        pair = wst[y]
        product = jnp.dot(
            jnp.concatenate(split(lam), axis=1),
            jnp.concatenate([pair, pair], axis=0),
            preferred_element_type=F32,
        )
        mixed = product[:, 0:levels] + product[:, levels:]
        flux = df[rows, :] * mixed
        st[rows, :] = mixed - 4.0 * flux
        fb[pl.ds(row_at(step % 2, y), lon), :] = flux
        return flux

    def share(step, b, edge):
        for low, size, at in segments(b, edge):
            base = row_at(step % 2, low)
            part = pl.ds(at, size)
            xs[step % 2, 0, part, :] = fb[pl.ds(base, size, stride=wide), :]
            xs[step % 2, 1, part, :] = fb[pl.ds(base + lon - 1, size, stride=wide), :]
        for copy in x_copies(step, b):
            copy.start()

    def edge_block(step):
        if step:
            edges_in(step - 1, 0, True)
            halo(step - 1)
        for side, y in enumerate((0, lat - 1)):
            ys[step % 2, side] = section(step, y).astype(BF16)
        for copy in y_copies(step):
            copy.start()
        if step == 0:
            add_columns()
        for j in range(1, HALF):
            section(step, j)
            section(step, lat - 1 - j)
        share(step, 0, True)

    def inner_blocks(step, low, high):
        def one(b, carry):
            if step:
                edges_in(step - 1, b, False)
            for j in range(ROWS):
                section(step, HALF + (b - 1) * ROWS + j)
            share(step, b, False)
            return carry

        lax.fori_loop(low, high, one, 0)

    def finish_row(y):
        obuf[pl.ds(y * lon, lon), :] = advanced(STEPS - 1, y)

    def finish_inner(b, carry):
        edges_in(STEPS - 1, b, False)
        for j in range(ROWS):
            finish_row(HALF + (b - 1) * ROWS + j)
        return carry

    edge_block(0)
    lax.fori_loop(early, blocks, force_block, 0)
    inner_blocks(0, 1, blocks)
    edge_block(1)
    inner_blocks(1, 1, blocks)
    inner_blocks(2, 1, middle)
    edge_block(2)
    inner_blocks(2, middle, blocks)
    inner_blocks(3, 1, blocks)
    edge_block(3)
    lax.fori_loop(1, blocks, finish_inner, 0)
    edges_in(STEPS - 1, 0, True)
    for j in range(1, HALF):
        finish_row(j)
        finish_row(lat - 1 - j)
    for copy in sends:
        copy.wait_send()
    halo(STEPS - 1)
    finish_row(0)
    finish_row(lat - 1)


def store_kernel(rows_ref, out_hbm, sem):
    lon, lat, _ = out_hbm.shape

    def store(y):
        return pltpu.make_async_copy(
            rows_ref.at[pl.ds(y * lon, lon)], out_hbm.at[:, y, :], sem.at[y]
        )

    for y in range(lat):
        store(y).start()
    for y in range(lat):
        store(y).wait()


def solution(mesh):
    n_gx, n_gy = mesh.shape["gx"], mesh.shape["gy"]

    def shards(state, diffusion, vert_inverse, profiles, counts, cell_lon, cell_lat, weight_slot):
        lon, lat, levels = state.shape
        n_all = counts.shape[1]
        slots = n_all * CAP
        blocks = lat // ROWS
        wide = lon + 2 * PAD
        dma = pltpu.SemaphoreType.DMA
        vmem = pl.BlockSpec(memory_space=pltpu.VMEM)
        obs = profiles.shape[0]
        out = pl.pallas_call(
            functools.partial(kernel, n_gx, n_gy),
            out_shape=pltpu.VMEM((lat * lon, levels), F32),
            in_specs=[pl.BlockSpec(memory_space=pltpu.HBM)] * 8,
            out_specs=vmem,
            scratch_shapes=[
                pltpu.VMEM((obs, levels), BF16),
                pltpu.VMEM((1, n_all), jnp.int32),
                pltpu.VMEM((1, obs), jnp.int32),
                pltpu.VMEM((1, obs), jnp.int32),
                pltpu.VMEM((2, obs), jnp.int32),
                pltpu.VMEM((lat * lon, levels), F32),
                pltpu.VMEM((lat * lon, levels), F32),
                pltpu.VMEM((lat, levels, levels), F32),
                pltpu.VMEM((lat, levels, 2 * levels), BF16),
                pltpu.VMEM((2 * (lat + 2) * wide, levels), F32),
                pltpu.VMEM((n_all, CAP, levels), BF16),
                pltpu.VMEM((n_all, 1, levels), F32),
                pltpu.VMEM((n_all, CAP, levels), BF16),
                pltpu.VMEM((n_all, 1, levels), F32),
                pltpu.VMEM((lon, slots), BF16),
                pltpu.VMEM((slots, 2 * levels), BF16),
                pltpu.VMEM((slots, 2 * levels), BF16),
                pltpu.VMEM((lat, levels), F32),
                pltpu.VMEM((lat, levels), F32),
                pltpu.VMEM((lon, levels), F32),
                pltpu.VMEM((lon, levels), BF16),
                pltpu.VMEM((lon, levels), BF16),
                pltpu.VMEM((PAD, levels), F32),
                pltpu.VMEM((PAD, levels), F32),
                pltpu.VMEM((2, 2, lat, levels), F32),
                pltpu.VMEM((STEPS, 2, lat, levels), F32),
                pltpu.VMEM((2, 2, lon, levels), BF16),
                pltpu.VMEM((STEPS, 2, lon, levels), BF16),
                dma((5,)), dma((blocks,)), dma((lat,)), dma((lat,)),
                dma((n_all,)), dma((n_all,)), dma((n_all,)), dma((n_all,)),
                dma((3,)), dma((3,)),
                dma((STEPS, 2, blocks)), dma((STEPS, 2, blocks)),
                dma((STEPS, 2)), dma((STEPS, 2)),
            ],
            compiler_params=pltpu.CompilerParams(
                collective_id=0, has_side_effects=True, vmem_limit_bytes=VMEM_LIMIT
            ),
            name="adjoint",
        )(
            *[
                pltpu.with_memory_space_constraint(x, pltpu.HBM)
                for x in (
                    profiles, counts, cell_lon[None], cell_lat[None], weight_slot,
                    state, diffusion, vert_inverse,
                )
            ]
        )
        return pl.pallas_call(
            store_kernel,
            out_shape=jax.ShapeDtypeStruct((lon, lat, levels), F32),
            in_specs=[vmem],
            out_specs=pl.BlockSpec(memory_space=pl.ANY),
            scratch_shapes=[dma((lat,))],
            compiler_params=pltpu.CompilerParams(vmem_limit_bytes=8 * 1024 * 1024),
            name="store",
        )(pltpu.with_memory_space_constraint(out, pltpu.VMEM))

    return jax.shard_map(
        shards,
        mesh=mesh,
        in_specs=(
            P("gx", "gy", None),
            P("gx", "gy", None),
            P("gy", None, None),
            P(("gx", "gy"), None),
            P(("gx", "gy"), None),
            P(("gx", "gy")),
            P(("gx", "gy")),
            P(None, ("gx", "gy")),
        ),
        out_specs=P("gx", "gy", None),
        check_vma=False,
    )
```

```python
import functools

import jax
import jax.numpy as jnp
from jax import lax
from jax.experimental import pallas as pl
from jax.experimental.pallas import tpu as pltpu
from jax.sharding import PartitionSpec as P

CAP = 16
STEPS = 4
SLOTS = 64
PAD = 8
ROWS = 8
HALF = ROWS // 2
FIELDS = 4
F32 = jnp.float32
BF16 = jnp.bfloat16
MESH = pl.DeviceIdType.MESH
VMEM_LIMIT = 48 * 1024 * 1024


def split(value):
    upper = value.astype(BF16)
    return upper, (value - upper.astype(F32)).astype(BF16)


def iota(shape, axis):
    return lax.broadcasted_iota(jnp.int32, shape, axis)


def kernel(
    n_gx, n_gy,
    prof_hbm, counts_hbm, lon_hbm, lat_hbm, slot_hbm, state_hbm, diff_hbm, inv_hbm, obuf,
    prof_ref, counts_ref, lon_ref, lat_ref, slot_ref, st, df, wf, wst, fb, msg, mmsg, recv, mrecv, wx, upper, lower,
    col_send, col_recv, near_row, row_send, row_recv, corner_send, corner_recv,
    xs, xr, ys, yr,
    small_sem, w_sem, st_sem, df_sem, v_send, v_recv, m_send, m_recv,
    f_send, f_recv, x_send, x_recv, y_send, y_recv,
):
    lon, lat, levels = state_hbm.shape
    n_all = n_gx * n_gy
    slots = n_all * CAP
    obs = prof_ref.shape[0]
    blocks = lat // ROWS
    wide = lon + 2 * PAD
    gx, gy = lax.axis_index("gx"), lax.axis_index("gy")
    me = gx * n_gy + gy
    gx_up, gx_down = lax.rem(gx + 1, n_gx), lax.rem(gx + n_gx - 1, n_gx)
    gy_up, gy_down = lax.rem(gy + 1, n_gy), lax.rem(gy + n_gy - 1, n_gy)
    east, west, north, south = (gx_up, gy), (gx_down, gy), (gx, gy_up), (gx, gy_down)

    small_loads = [
        pltpu.make_async_copy(src, dst, small_sem.at[i])
        for i, (src, dst) in enumerate(
            (
                (counts_hbm, counts_ref), (prof_hbm, prof_ref), (lon_hbm, lon_ref),
                (lat_hbm, lat_ref), (slot_hbm, slot_ref),
            )
        )
    ]
    for load in small_loads:
        load.start()

    columns = [lax.rem(gx + d, n_gx) for d in range(n_gx)]
    lines = [lax.rem(gy + d, n_gy) for d in range(n_gy)]
    peers = [(column, line) for column in columns for line in lines]

    barrier = pltpu.get_barrier_semaphore()
    for peer in peers[1:]:
        pl.semaphore_signal(barrier, inc=1, device_id=peer, device_id_type=MESH)

    for load in small_loads:
        load.wait()

    w_loads = [
        pltpu.make_async_copy(
            inv_hbm.at[pl.ds(b * ROWS, ROWS)], wf.at[pl.ds(b * ROWS, ROWS)], w_sem.at[b]
        )
        for b in range(blocks)
    ]
    for load in w_loads:
        load.start()
    for y in range(lat):
        rows = pl.ds(y * lon, lon)
        pltpu.make_async_copy(state_hbm.at[:, y, :], st.at[rows], st_sem.at[y]).start()
    for y in range(lat):
        rows = pl.ds(y * lon, lon)
        pltpu.make_async_copy(diff_hbm.at[:, y, :], df.at[rows], df_sem.at[y]).start()

    count_row = counts_ref[...].astype(F32)
    dest, lane = iota((n_all, n_all), 0), iota((n_all, n_all), 1)
    start = jnp.sum(jnp.where(lane < dest, count_row, 0.0), axis=1, keepdims=True)
    count = jnp.sum(jnp.where(lane == dest, count_row, 0.0), axis=1, keepdims=True)
    position = iota((n_all, obs), 1).astype(F32)
    inside = jnp.where((position >= start) & (position < start + count), 1.0, 0.0)
    owner = iota((n_all, obs), 0).astype(F32)
    slot_of = jnp.sum(inside * (position - start), axis=0, keepdims=True)
    code = jnp.sum(inside * owner, axis=0, keepdims=True) * CAP + slot_of
    selector = jnp.where(iota((slots, obs), 0) == code.astype(jnp.int32), 1.0, 0.0).astype(BF16)
    msg[...] = (
        jnp.dot(selector, prof_ref[...], preferred_element_type=F32)
        .astype(BF16)
        .reshape(n_all, CAP, levels)
    )
    field = iota((levels, obs), 0)
    meta = jnp.where(field < CAP, lon_ref[...].astype(F32), lat_ref[...].astype(F32))
    meta = jnp.where(field < 2 * CAP, meta, slot_ref[0:1, :].astype(F32))
    meta = jnp.where(field < 3 * CAP, meta, slot_ref[1:2, :].astype(F32))
    meta = jnp.where(field % CAP == slot_of.astype(jnp.int32), meta, 0.0).astype(BF16)
    mmsg[...] = lax.dot_general(
        inside.astype(BF16), meta, (((1,), (1,)), ((), ())), preferred_element_type=F32
    ).reshape(n_all, 1, levels)

    pl.semaphore_wait(barrier, n_all - 1)

    sends = []
    for k, (column, line) in enumerate(peers[1:], 1):
        other = column * n_gy + line
        for src, dst, send_sem, recv_sem in (
            (msg, recv, v_send, v_recv), (mmsg, mrecv, m_send, m_recv)
        ):
            sends.append(
                pltpu.make_async_remote_copy(
                    src_ref=src.at[other], dst_ref=dst.at[k],
                    send_sem=send_sem.at[0], recv_sem=recv_sem.at[0],
                    device_id=(column, line), device_id_type=MESH,
                )
            )
    for copy in sends:
        copy.start()
    recv[0] = msg[me]
    mrecv[0] = mmsg[me]

    for b in range(blocks):
        w_loads[b].wait()

        def pairs(i, carry):
            for j in range(2):
                y = b * ROWS + 2 * i + j
                wst[y] = jnp.concatenate(split(wf[y]), axis=1)
            return carry

        lax.fori_loop(0, ROWS // 2, pairs, 0)

    for y in range(lat):
        rows = pl.ds(y * lon, lon)
        pltpu.make_async_copy(state_hbm.at[:, y, :], st.at[rows], st_sem.at[y]).wait()

    for y in range(lat):
        rows = pl.ds(y * lon, lon)
        pltpu.make_async_copy(diff_hbm.at[:, y, :], df.at[rows], df_sem.at[y]).wait()

    pick = iota((CAP, levels), 1) - 3 * CAP == iota((CAP, levels), 0)
    for dst, sem in ((recv, v_recv), (mrecv, m_recv)):
        part = dst.at[pl.ds(1, n_all - 1)]
        pltpu.make_async_copy(part, part, sem.at[0]).wait()
    for k in range(n_all):
        here = slice(k * CAP, (k + 1) * CAP)
        frac_y = (
            jnp.sum(jnp.where(pick, mrecv[k], 0.0), axis=1, keepdims=True) / SLOTS
        )
        values = recv[k].astype(F32)
        far = values * frac_y
        near_terms, far_terms = split(values - far), split(far)
        upper[here, 0:levels], lower[here, 0:levels] = near_terms
        upper[here, levels:], lower[here, levels:] = far_terms

    table = mrecv[...].reshape(n_all, levels)
    spread = jnp.where(iota((n_all, slots), 1) // CAP == iota((n_all, slots), 0), 1.0, 0.0)
    wide_table = lax.dot_general(
        table.astype(BF16), spread.astype(BF16), (((0,), (0,)), ((), ())),
        preferred_element_type=F32,
    )
    own = iota((levels, slots), 0) % CAP == iota((levels, slots), 1) % CAP
    wide_table = jnp.where(own, wide_table, 0.0)
    lon_row, lat_row, frac_row = [
        jnp.sum(wide_table[f * CAP : (f + 1) * CAP], axis=0, keepdims=True) for f in range(3)
    ]
    frac_row = frac_row / SLOTS
    x_ids = iota((lon, slots), 0).astype(F32)
    wx_f = jnp.where(x_ids == lon_row, 1.0 - frac_row, 0.0) + jnp.where(
        x_ids == lon_row + 1.0, frac_row, 0.0
    )
    wx[...] = wx_f.astype(BF16)
    def weighted(rows):
        return jnp.dot(rows, upper[...], preferred_element_type=F32) + jnp.dot(
            rows, lower[...], preferred_element_type=F32
        )

    last = jnp.where(lon_row == lon - 1.0, frac_row, 0.0)
    y_ids = iota((lat, slots), 0).astype(F32)
    edges = weighted(
        jnp.concatenate(
            [
                jnp.where(y_ids == lat_row, last, 0.0).astype(BF16),
                jnp.where(lat_row == lat - 1.0, wx_f, 0.0).astype(BF16),
            ],
            axis=0,
        )
    )
    far_col = edges[0:lat, levels:]
    shifted = jnp.where(iota((lat, levels), 0) == 0, 0.0, pltpu.roll(far_col, 1, 0))
    col_send[...] = edges[0:lat, 0:levels] + shifted
    corner_send[...] = pltpu.roll(far_col, 1, 0)[0:PAD]
    row_send[...] = edges[lat:, levels:].astype(BF16)
    near_row[...] = edges[lat:, 0:levels]
    f_copies = [
        pltpu.make_async_remote_copy(
            src_ref=src, dst_ref=dst, send_sem=f_send.at[i], recv_sem=f_recv.at[i],
            device_id=device, device_id_type=MESH,
        )
        for i, (src, dst, device) in enumerate(
            (
                (col_send, col_recv, east),
                (row_send, row_recv, north),
                (corner_send, corner_recv, (gx_up, gy_up)),
            )
        )
    ]
    for copy in f_copies:
        copy.start()

    done_row = lat - HALF - 1

    def force(runs, edge):
        parts = []
        for low, size in runs:
            for j in range(size):
                y = low + j
                if not edge:
                    y = jnp.where(y == done_row, -1, y).astype(F32)
                hot = jnp.where(lat_row == y, 1.0, 0.0).astype(BF16)
                parts.append(wx[...] * hot)
        total = weighted(jnp.concatenate(parts, axis=0))
        at = 0
        for low, size in runs:
            for j in range(size + 1):
                rows = pl.ds((low + j) * lon, lon)
                add = None
                if j < size:
                    add = total[at * lon : (at + 1) * lon, 0:levels]
                if j:
                    behind = total[(at - 1) * lon : at * lon, levels:]
                    add = behind if add is None else add + behind
                st[rows, :] = st[rows, :] + add
                at = at + 1 if j < size else at

    def force_block(b, carry):
        force([(HALF + (b - 1) * ROWS, ROWS)], False)
        return carry

    force([(0, HALF), (done_row, HALF)], True)
    final = pl.ds((lat - 1) * lon, lon)
    st[final, :] = st[final, :] + near_row[...]
    early = (3 * blocks) // 4
    middle = (3 * blocks) // 4
    lax.fori_loop(1, early, force_block, 0)
    for copy in f_copies:
        copy.wait()
    first_x = iota((lon, levels), 0) == 0

    def add_column(y):
        rows = pl.ds(y * lon, lon)
        st[rows, :] = st[rows, :] + jnp.where(first_x, col_recv[y : y + 1, :], 0.0)

    def add_columns():
        y = iota((lat, levels), 0)
        edge = pl.ds(0, lat, stride=lon)
        st[edge, :] = st[edge, :] + jnp.where((y > 0) & (y < lat - 1), col_recv[...], 0.0)

    st[0:lon, :] = st[0:lon, :] + jnp.where(
        gy > 0, row_recv[...].astype(F32) + jnp.where(first_x, corner_recv[0:1, :], 0.0), 0.0
    )
    add_column(0)
    add_column(lat - 1)

    def row_at(parity, y):
        return (parity * (lat + 2) + y + 1) * wide + PAD

    def x_copies(step, b):
        copies = []
        for side, device in ((0, west), (1, east)):
            copies.append(
                pltpu.make_async_remote_copy(
                    src_ref=xs.at[step % 2, side, pl.ds(b * ROWS, ROWS)],
                    dst_ref=xr.at[step, 1 - side, pl.ds(b * ROWS, ROWS)],
                    send_sem=x_send.at[step, side, b], recv_sem=x_recv.at[step, 1 - side, b],
                    device_id=device, device_id_type=MESH,
                )
            )
        return copies

    def y_copies(step):
        return [
            pltpu.make_async_remote_copy(
                src_ref=ys.at[step % 2, side], dst_ref=yr.at[step, 1 - side],
                send_sem=y_send.at[step, side], recv_sem=y_recv.at[step, 1 - side],
                device_id=device, device_id_type=MESH,
            )
            for side, device in ((0, south), (1, north))
        ]

    def segments(b, edge):
        if edge:
            return [(0, HALF, 0), (lat - HALF, HALF, HALF)]
        return [(HALF + (b - 1) * ROWS, ROWS, b * ROWS)]

    def edges_in(step, b, edge):
        for copy in x_copies(step, b):
            copy.wait()
        for low, size, at in segments(b, edge):
            base = row_at(step % 2, low)
            part = pl.ds(at, size)
            fb[pl.ds(base - 1, size, stride=wide), :] = xr[step, 0, part, :]
            fb[pl.ds(base + lon, size, stride=wide), :] = xr[step, 1, part, :]

    def advanced(step, y):
        base = row_at(step % 2, y)
        total = fb[pl.ds(base - 1, lon), :] + fb[pl.ds(base + 1, lon), :]
        total = total + (fb[pl.ds(base - wide, lon), :] + fb[pl.ds(base + wide, lon), :])
        return st[pl.ds(y * lon, lon), :] + total

    def halo(step):
        for copy in y_copies(step):
            copy.wait()
        parity = step % 2
        fb[pl.ds(row_at(parity, -1), lon), :] = jnp.where(gy > 0, yr[step, 0].astype(F32), 0.0)
        fb[pl.ds(row_at(parity, lat), lon), :] = jnp.where(
            gy < n_gy - 1, yr[step, 1].astype(F32), 0.0
        )

    def section(step, y):
        rows = pl.ds(y * lon, lon)
        lam = st[rows, :] if step == 0 else advanced(step - 1, y)
        pair = wst[y]
        product = jnp.dot(
            jnp.concatenate(split(lam), axis=1),
            jnp.concatenate([pair, pair], axis=0),
            preferred_element_type=F32,
        )
        mixed = product[:, 0:levels] + product[:, levels:]
        flux = df[rows, :] * mixed
        st[rows, :] = mixed - 4.0 * flux
        fb[pl.ds(row_at(step % 2, y), lon), :] = flux
        return flux

    def share(step, b, edge):
        for low, size, at in segments(b, edge):
            base = row_at(step % 2, low)
            part = pl.ds(at, size)
            xs[step % 2, 0, part, :] = fb[pl.ds(base, size, stride=wide), :]
            xs[step % 2, 1, part, :] = fb[pl.ds(base + lon - 1, size, stride=wide), :]
        for copy in x_copies(step, b):
            copy.start()

    def edge_block(step):
        if step:
            edges_in(step - 1, 0, True)
            halo(step - 1)
        for side, y in enumerate((0, lat - 1)):
            ys[step % 2, side] = section(step, y).astype(BF16)
        for copy in y_copies(step):
            copy.start()
        if step == 0:
            add_columns()
        for j in range(1, HALF):
            section(step, j)
            section(step, lat - 1 - j)
        share(step, 0, True)

    def inner_blocks(step, low, high):
        def one(b, carry):
            if step:
                edges_in(step - 1, b, False)
            for j in range(ROWS):
                section(step, HALF + (b - 1) * ROWS + j)
            share(step, b, False)
            return carry

        lax.fori_loop(low, high, one, 0)

    def finish_row(y):
        obuf[pl.ds(y * lon, lon), :] = advanced(STEPS - 1, y)

    def finish_inner(b, carry):
        edges_in(STEPS - 1, b, False)
        for j in range(ROWS):
            finish_row(HALF + (b - 1) * ROWS + j)
        return carry

    edge_block(0)
    lax.fori_loop(early, blocks, force_block, 0)
    inner_blocks(0, 1, blocks)
    edge_block(1)
    inner_blocks(1, 1, blocks)
    inner_blocks(2, 1, middle)
    edge_block(2)
    inner_blocks(2, middle, blocks)
    inner_blocks(3, 1, blocks)
    edge_block(3)
    lax.fori_loop(1, blocks, finish_inner, 0)
    edges_in(STEPS - 1, 0, True)
    for j in range(1, HALF):
        finish_row(j)
        finish_row(lat - 1 - j)
    for src, sem in ((msg, v_send), (mmsg, m_send)):
        part = src.at[pl.ds(1, n_all - 1)]
        pltpu.make_async_copy(part, part, sem.at[0]).wait()
    halo(STEPS - 1)
    finish_row(0)
    finish_row(lat - 1)


def store_kernel(rows_ref, out_hbm, sem):
    lon, lat, _ = out_hbm.shape

    def store(y):
        return pltpu.make_async_copy(
            rows_ref.at[pl.ds(y * lon, lon)], out_hbm.at[:, y, :], sem.at[0]
        )

    for y in range(lat):
        store(y).start()
    pltpu.make_async_copy(rows_ref, rows_ref, sem.at[0]).wait()


def solution(mesh):
    n_gx, n_gy = mesh.shape["gx"], mesh.shape["gy"]

    def shards(state, diffusion, vert_inverse, profiles, counts, cell_lon, cell_lat, weight_slot):
        lon, lat, levels = state.shape
        n_all = counts.shape[1]
        slots = n_all * CAP
        blocks = lat // ROWS
        wide = lon + 2 * PAD
        dma = pltpu.SemaphoreType.DMA
        vmem = pl.BlockSpec(memory_space=pltpu.VMEM)
        obs = profiles.shape[0]
        out = pl.pallas_call(
            functools.partial(kernel, n_gx, n_gy),
            out_shape=pltpu.VMEM((lat * lon, levels), F32),
            in_specs=[pl.BlockSpec(memory_space=pltpu.HBM)] * 8,
            out_specs=vmem,
            scratch_shapes=[
                pltpu.VMEM((obs, levels), BF16),
                pltpu.VMEM((1, n_all), jnp.int32),
                pltpu.VMEM((1, obs), jnp.int32),
                pltpu.VMEM((1, obs), jnp.int32),
                pltpu.VMEM((2, obs), jnp.int32),
                pltpu.VMEM((lat * lon, levels), F32),
                pltpu.VMEM((lat * lon, levels), F32),
                pltpu.VMEM((lat, levels, levels), F32),
                pltpu.VMEM((lat, levels, 2 * levels), BF16),
                pltpu.VMEM((2 * (lat + 2) * wide, levels), F32),
                pltpu.VMEM((n_all, CAP, levels), BF16),
                pltpu.VMEM((n_all, 1, levels), F32),
                pltpu.VMEM((n_all, CAP, levels), BF16),
                pltpu.VMEM((n_all, 1, levels), F32),
                pltpu.VMEM((lon, slots), BF16),
                pltpu.VMEM((slots, 2 * levels), BF16),
                pltpu.VMEM((slots, 2 * levels), BF16),
                pltpu.VMEM((lat, levels), F32),
                pltpu.VMEM((lat, levels), F32),
                pltpu.VMEM((lon, levels), F32),
                pltpu.VMEM((lon, levels), BF16),
                pltpu.VMEM((lon, levels), BF16),
                pltpu.VMEM((PAD, levels), F32),
                pltpu.VMEM((PAD, levels), F32),
                pltpu.VMEM((2, 2, lat, levels), F32),
                pltpu.VMEM((STEPS, 2, lat, levels), F32),
                pltpu.VMEM((2, 2, lon, levels), BF16),
                pltpu.VMEM((STEPS, 2, lon, levels), BF16),
                dma((5,)), dma((blocks,)), dma((lat,)), dma((lat,)),
                dma((1,)), dma((1,)), dma((1,)), dma((1,)),
                dma((3,)), dma((3,)),
                dma((STEPS, 2, blocks)), dma((STEPS, 2, blocks)),
                dma((STEPS, 2)), dma((STEPS, 2)),
            ],
            compiler_params=pltpu.CompilerParams(
                collective_id=0, has_side_effects=True, vmem_limit_bytes=VMEM_LIMIT
            ),
            name="adjoint",
        )(
            *[
                pltpu.with_memory_space_constraint(x, pltpu.HBM)
                for x in (
                    profiles, counts, cell_lon[None], cell_lat[None], weight_slot,
                    state, diffusion, vert_inverse,
                )
            ]
        )
        return pl.pallas_call(
            store_kernel,
            out_shape=jax.ShapeDtypeStruct((lon, lat, levels), F32),
            in_specs=[vmem],
            out_specs=pl.BlockSpec(memory_space=pl.ANY),
            scratch_shapes=[dma((1,))],
            compiler_params=pltpu.CompilerParams(vmem_limit_bytes=8 * 1024 * 1024),
            name="store",
        )(pltpu.with_memory_space_constraint(out, pltpu.VMEM))

    return jax.shard_map(
        shards,
        mesh=mesh,
        in_specs=(
            P("gx", "gy", None),
            P("gx", "gy", None),
            P("gy", None, None),
            P(("gx", "gy"), None),
            P(("gx", "gy"), None),
            P(("gx", "gy")),
            P(("gx", "gy")),
            P(None, ("gx", "gy")),
        ),
        out_specs=P("gx", "gy", None),
        check_vma=False,
    )
```
